32 devices in a mesh: beam: 2 (over x), chan: 16 (over z, y, core).
Axes of the slice: x: 2, y: 2, z: 4, core: 2. Of those that a mesh axis runs over, the one named last changes fastest.
Arguments:
- spectra: float32 [4096, 1024], P(('beam', 'chan')), parts along dimension 0, may hold values from -6 to 6
- chan_delay: int32 [2048, 32], P('chan'), may hold values from 0 to 63
- window_base: int32 [16, 64], P(None, 'chan'), may hold values from 0 to 28
- trial_offset: int32 [256, 64], P('chan'), may hold values from 0 to 3
- shift_blocks: int32 [256], P('chan'), may hold values from 0 to 7
- template_len: int32 [8], replicated, may hold values from 1 to 128
Outputs:
- scores: float32 [512, 8, 1024], P(('beam', 'chan')), parts along dimension 0
The draws below stay inside these ranges and needn't reach their ends.
There are 2 independent parts, one for each index of `beam`. The reference program is written for one: setup_inputs(seed, part) draws one part's arguments, and reference() takes and returns one part's arrays. A program takes and returns all parts, laid end to end along the dimension named above; an argument that names none is the same for every part. Nothing has to cross between parts.
All inputs are finite; a program needn't handle non-finite values.
Results may differ from the reference program's by a relative error of at most 0.0032.
Values may be sent and summed in bfloat16 or wider, within the bound.
No kernel may reach another device: no remote copies, remote signals or barrier semaphores. Data moves between devices by JAX's collectives and lax.ppermute only.
A program may use at most 64 MiB of HBM per device.

```python
import jax
import jax.numpy as jnp
from jax import lax

SUB_CH = 32
NDELAY = 32
MAXD = 64
SPAN = 4
TRIAL_DEV = 16
SAMPLES = 1024
BLOCK = 128
NTEMP = 8
SHIFT_MAX = 7
CHANS = 2048
SUBBANDS = 64
TRIALS = 256
OWNERS = 16


def place_ends(array, rng, smallest, largest):
    extent = array.shape
    place = [jax.random.randint(jax.random.fold_in(rng, axis), (), 0, extent[axis]) for axis in range(len(extent))]
    array = array.at[tuple(place)].set(smallest)
    longest = extent.index(max(extent))
    place[longest] = (place[longest] + 1) % extent[longest]
    return array.at[tuple(place)].set(largest)


def steps_of(own_key, shape, shards, low, top_value):
    loudness, own = 1.0, jax.random.fold_in(own_key, 6)
    for dim, parts in shards:
        heights = jnp.exp(jax.random.uniform(jax.random.fold_in(own, dim), (parts,), jnp.float32, low / len(shards), top_value / len(shards)))
        loudness = loudness * jnp.repeat(heights, shape[dim] // parts).reshape([-1 if axis == dim else 1 for axis in range(len(shape))])
    return loudness


def bell_draw(own_key, shape, scale, reach, cuts=(), kind=jnp.bfloat16):
    gain = steps_of(own_key, shape, cuts, -0.22, 0.18) if cuts else 1.0
    result = jax.random.normal(own_key, shape, jnp.float32) * scale * gain
    return jnp.minimum(jnp.maximum(result, -reach), reach).astype(kind)


def setup_inputs(seed: int = 0, part: int = 0) -> dict:
    key_of = jax.random.split(jax.random.key(seed), 7)
    own_keys = jax.random.split(jax.random.fold_in(key_of[6], part), 7)
    spectra = bell_draw(own_keys[0], (CHANS, SAMPLES), 1.0, 6.0, ((0, 16),), jnp.float32)
    chan_delay = place_ends(jax.random.randint(key_of[1], (CHANS, NDELAY), 0, MAXD), jax.random.fold_in(key_of[1], 1), 0, MAXD - 1).astype(jnp.int32)
    window_base = place_ends(jax.random.randint(key_of[2], (OWNERS, SUBBANDS), 0, NDELAY - SPAN + 1), jax.random.fold_in(key_of[2], 1), 0, NDELAY - SPAN).astype(jnp.int32)
    trial_offset = place_ends(jax.random.randint(key_of[3], (TRIALS, SUBBANDS), 0, SPAN), jax.random.fold_in(key_of[3], 1), 0, SPAN - 1).astype(jnp.int32)
    shift_blocks = place_ends(jax.random.randint(key_of[4], (TRIALS,), 0, SHIFT_MAX + 1), jax.random.fold_in(key_of[4], 1), 0, SHIFT_MAX).astype(jnp.int32)
    template_len = place_ends(jax.random.randint(key_of[5], (NTEMP,), 1, BLOCK + 1), jax.random.fold_in(key_of[5], 1), 1, BLOCK).astype(jnp.int32)
    return {"spectra": spectra, "chan_delay": chan_delay, "window_base": window_base, "trial_offset": trial_offset, "shift_blocks": shift_blocks, "template_len": template_len}


def reference(spectra, chan_delay, window_base, trial_offset, shift_blocks, template_len):
    channels, samples = spectra.shape
    sample_index = jnp.arange(samples, dtype=jnp.int32)

    def one_delay(unused, column):
        source = sample_index[None, :] - column[:, None]
        picked = jnp.take_along_axis(spectra, jnp.clip(source, 0, samples - 1), axis=1)
        picked = jnp.where(source >= 0, picked, jnp.zeros_like(picked))
        summed = picked.reshape(channels // SUB_CH, SUB_CH, samples).sum(axis=1) * SUB_CH ** (-0.5)
        return (unused, summed.astype(jnp.bfloat16))
    _, delay_rows = lax.scan(one_delay, jnp.zeros((), jnp.float32), jnp.transpose(chan_delay))
    trial_delay = (jnp.repeat(window_base, TRIAL_DEV, axis=0) + trial_offset).astype(jnp.int32)

    def add_band(total, band):
        index_col, rows_band = band
        picked = jnp.take(rows_band, index_col, axis=0).astype(jnp.float32)
        return (total + picked, None)
    total, _ = lax.scan(add_band, jnp.zeros((TRIALS, samples), jnp.float32), (jnp.transpose(trial_delay), jnp.transpose(delay_rows, (1, 0, 2))))
    dedispersed = total * SUBBANDS ** (-0.5)
    block_count = samples // BLOCK
    blocks = dedispersed.reshape(TRIALS, block_count, BLOCK)
    source = jnp.arange(block_count, dtype=jnp.int32)[None, :] + shift_blocks[:, None]
    shifted = jnp.take_along_axis(blocks, jnp.clip(source, 0, block_count - 1)[:, :, None], axis=1)
    shifted = jnp.where((source < block_count)[:, :, None], shifted, jnp.zeros_like(shifted))
    flat_shifted = shifted.reshape(TRIALS, samples)
    padded = jnp.pad(flat_shifted, ((0, 0), (1, BLOCK)))
    running = jnp.cumsum(padded, axis=1)
    lower = running[:, :samples]
    outputs = []
    for which_one in range(NTEMP):
        length_now = template_len[which_one]
        upper = lax.dynamic_slice_in_dim(running, length_now.astype(jnp.int32), samples, 1)
        outputs.append((upper - lower) * lax.rsqrt(length_now.astype(jnp.float32)))
    return jnp.stack(outputs, axis=1)
```

```python
import functools

import jax
import jax.numpy as jnp
from jax import lax
from jax.experimental import pallas as pl
from jax.experimental.pallas import tpu as pltpu
from jax.sharding import PartitionSpec as P

SUB_CH = 32
NDELAY = 32
MAXD = 64
SPAN = 4
BLOCK = 128
FINE = 8
COARSE = MAXD // FINE


def later(x, amount):
    if amount == 0:
        return x
    moved = pltpu.roll(x, amount, 1)
    lane = lax.broadcasted_iota(jnp.int32, (x.shape[0], BLOCK), 1)
    first = jnp.where(lane >= amount, moved[:, :BLOCK], 0.0)
    return jnp.concatenate([first, moved[:, BLOCK:]], axis=1)


def rows_kernel(spectra_ref, delay_ref, base_ref, out_ref, high_ref, low_ref, sums_ref, rows_ref):
    channels, samples = spectra_ref.shape
    bands = channels // SUB_CH
    owners = base_ref.shape[0]
    delay_of = jnp.transpose(delay_ref[...])
    lane = lax.broadcasted_iota(jnp.int32, (NDELAY, channels), 1)
    fine_per_tile = channels // SUB_CH
    for band in range(bands):
        mine = spectra_ref[band * SUB_CH : (band + 1) * SUB_CH, :]
        for fine in range(FINE):
            moved = later(mine, fine)
            high = moved.astype(jnp.bfloat16)
            low = (moved - high.astype(jnp.float32)).astype(jnp.bfloat16)
            high_ref[fine * SUB_CH : (fine + 1) * SUB_CH, :] = high
            low_ref[fine * SUB_CH : (fine + 1) * SUB_CH, :] = low
        tiled = jnp.where(lane // SUB_CH == band, delay_of, 0)
        step = SUB_CH
        while step < channels:
            tiled = tiled + pltpu.roll(tiled, step, 1)
            step *= 2
        tables = []
        for coarse in range(COARSE):
            parts = []
            for start in range(0, FINE, fine_per_tile):
                wanted = coarse * FINE + start + lane // SUB_CH
                parts.append(jnp.where(tiled == wanted, 1.0, 0.0).astype(jnp.bfloat16))
            tables.append(jnp.concatenate(parts, axis=1))
        table = jnp.concatenate(tables, axis=0)
        sums_ref[...] = jnp.dot(table, high_ref[...], preferred_element_type=jnp.float32) + jnp.dot(
            table, low_ref[...], preferred_element_type=jnp.float32
        )
        total = sums_ref[:NDELAY, :]
        for coarse in range(1, COARSE):
            total = total + later(sums_ref[coarse * NDELAY : (coarse + 1) * NDELAY, :], coarse * FINE)
        rows_ref[band * NDELAY : (band + 1) * NDELAY, :] = (total * SUB_CH ** (-0.5)).astype(jnp.bfloat16)
    width = bands * NDELAY
    lane = lax.broadcasted_iota(jnp.int32, (owners, width), 1)
    base = jnp.zeros((owners, width), jnp.int32)
    for band in range(bands):
        base = jnp.where(lane // NDELAY == band, base_ref[:, band : band + 1], base)
    count = bands * SPAN
    lane = lax.broadcasted_iota(jnp.int32, (count, width), 1)
    place = lax.broadcasted_iota(jnp.int32, (count, width), 0)
    within = jnp.where(place // SPAN == lane // NDELAY, lane % NDELAY - place % SPAN, -1)
    group = min(owners, 16)
    rows = rows_ref[...]
    for start in range(0, owners, group):
        picks = [jnp.where(base[o : o + 1, :] == within, 1.0, 0.0).astype(jnp.bfloat16) for o in range(start, start + group)]
        picked = jnp.dot(jnp.concatenate(picks, axis=0), rows, preferred_element_type=jnp.float32)
        out_ref[start * count : (start + group) * count, :] = picked.astype(jnp.bfloat16)


def column(row, size):
    same = lax.broadcasted_iota(jnp.int32, (size, size), 0) == lax.broadcasted_iota(jnp.int32, (size, size), 1)
    return jnp.sum(jnp.where(same, row.astype(jnp.float32), 0.0), axis=1, keepdims=True).astype(jnp.int32)


def scores_kernel(stacked_ref, offset_ref, shift_ref, length_ref, out_ref, prefix_ref, after_ref):
    trials, subbands = offset_ref.shape
    samples = stacked_ref.shape[1]
    blocks = samples // BLOCK
    templates = length_ref.shape[1]
    spread = lax.broadcasted_iota(jnp.int32, (subbands, subbands * SPAN), 1) // SPAN
    spread = (spread == lax.broadcasted_iota(jnp.int32, (subbands, subbands * SPAN), 0)).astype(jnp.bfloat16)
    wide = jnp.dot(offset_ref[...].astype(jnp.bfloat16), spread, preferred_element_type=jnp.float32)
    span_of = (lax.broadcasted_iota(jnp.int32, wide.shape, 1) % SPAN).astype(jnp.float32)
    picker = jnp.where(wide == span_of, 1.0, 0.0).astype(jnp.bfloat16)
    summed = jnp.dot(picker, stacked_ref[...], preferred_element_type=jnp.float32) * subbands ** (-0.5)
    current = [summed[:, b * BLOCK : (b + 1) * BLOCK] for b in range(blocks)]
    shift = jnp.broadcast_to(column(shift_ref[...], trials), (trials, BLOCK))
    bit = 1
    while bit < blocks:
        taken = (shift & bit) != 0
        current = [jnp.where(taken, current[b + bit] if b + bit < blocks else 0.0, current[b]) for b in range(blocks)]
        bit *= 2
    lane = lax.broadcasted_iota(jnp.int32, (trials, BLOCK), 1)
    before = jnp.zeros((trials, BLOCK), jnp.float32)
    for b in range(blocks):
        total = current[b]
        step = 1
        while step < BLOCK:
            total = total + jnp.where(lane >= step, pltpu.roll(total, step, 1), 0.0)
            step *= 2
        exclusive = total - current[b]
        prefix_ref[:, b * BLOCK : (b + 1) * BLOCK] = exclusive
        if b > 0:
            after_ref[:, (b - 1) * BLOCK : b * BLOCK] = exclusive + before
        before = jnp.broadcast_to(total[:, BLOCK - 1 :], (trials, BLOCK))
    after_ref[:, (blocks - 1) * BLOCK :] = before
    length = jnp.broadcast_to(column(length_ref[...], templates), (templates, BLOCK))
    lane = lax.broadcasted_iota(jnp.int32, (templates, BLOCK), 1)
    source = (lane + length) % BLOCK
    from_next = lane < length
    weight = lax.rsqrt(length.astype(jnp.float32))
    for b in range(blocks):
        for j in range(trials):
            here = jnp.broadcast_to(prefix_ref[j : j + 1, b * BLOCK : (b + 1) * BLOCK], (templates, BLOCK))
            there = jnp.broadcast_to(after_ref[j : j + 1, b * BLOCK : (b + 1) * BLOCK], (templates, BLOCK))
            ends = jnp.take_along_axis(jnp.where(from_next, there, here), source, axis=1)
            out_ref[j, :, b * BLOCK : (b + 1) * BLOCK] = (ends - here) * weight


def local(spectra, chan_delay, window_base, trial_offset, shift_blocks, template_len):
    channels, samples = spectra.shape
    owners = window_base.shape[0]
    bands = channels // SUB_CH
    trials, subbands = trial_offset.shape
    templates = template_len.shape[0]
    count = bands * SPAN
    windows = pl.pallas_call(
        rows_kernel,
        out_shape=jax.ShapeDtypeStruct((owners * count, samples), jnp.bfloat16),
        scratch_shapes=[
            pltpu.VMEM((FINE * SUB_CH, samples), jnp.bfloat16),
            pltpu.VMEM((FINE * SUB_CH, samples), jnp.bfloat16),
            pltpu.VMEM((COARSE * NDELAY, samples), jnp.float32),
            pltpu.VMEM((bands * NDELAY, samples), jnp.bfloat16),
        ],
        name="rows",
    )(spectra, chan_delay, window_base)
    stacked = lax.all_to_all(windows, "chan", split_axis=0, concat_axis=0, tiled=True)
    return pl.pallas_call(
        scores_kernel,
        out_shape=jax.ShapeDtypeStruct((trials, templates, samples), jnp.float32),
        scratch_shapes=[pltpu.VMEM((trials, samples), jnp.float32), pltpu.VMEM((trials, samples), jnp.float32)],
        name="scores",
    )(stacked, trial_offset, shift_blocks.reshape(1, trials), template_len.reshape(1, templates))


def solution(mesh):
    in_specs = (
        P(("beam", "chan"), None),
        P("chan", None),
        P(None, "chan"),
        P("chan", None),
        P("chan"),
        P(),
    )
    out_specs = P(("beam", "chan"), None, None)
    return jax.shard_map(local, mesh=mesh, in_specs=in_specs, out_specs=out_specs, check_vma=False)
```

```python
import jax
import jax.numpy as jnp
from jax import lax
from jax.experimental import pallas as pl
from jax.experimental.pallas import tpu as pltpu
from jax.sharding import PartitionSpec as P

SUB_CH = 32
NDELAY = 32
MAXD = 64
SPAN = 4
BLOCK = 128
FINE = 8
COARSE = MAXD // FINE
TILE = 256
HALF = 16


def later(x, amount):
    if amount == 0:
        return x
    moved = pltpu.roll(x, amount, 1)
    lane = lax.broadcasted_iota(jnp.int32, (x.shape[0], BLOCK), 1)
    first = jnp.where(lane >= amount, moved[:, :BLOCK], jnp.zeros((), x.dtype))
    return jnp.concatenate([first, moved[:, BLOCK:]], axis=1)


def column(row, size):
    same = lax.broadcasted_iota(jnp.int32, (size, size), 0) == lax.broadcasted_iota(jnp.int32, (size, size), 1)
    return jnp.sum(jnp.where(same, row.astype(jnp.float32), 0.0), axis=1, keepdims=True).astype(jnp.int32)


def rows_kernel(
    spectra_hbm, delay_hbm, base_hbm, offset_hbm, shift_hbm, length_hbm,
    windows_ref, picker_ref, shift_ref, length_ref,
    spectra_ref, delay_ref, base_ref, offset_in, shift_in, length_in,
    tables_ref, picks_ref, terms_ref, sums_ref, rows_ref, sems,
):
    channels, samples = spectra_ref.shape
    bands = channels // SUB_CH
    owners = base_ref.shape[1]
    depth = FINE * SUB_CH
    width = bands * NDELAY
    count = bands * SPAN

    small = [
        pltpu.make_async_copy(source, target, sems.at[bands + i])
        for i, (source, target) in enumerate(
            [(delay_hbm, delay_ref), (base_hbm, base_ref), (offset_hbm, offset_in), (shift_hbm, shift_in), (length_hbm, length_in)]
        )
    ]
    large = []
    for band in range(bands):
        part = pl.ds(band * SUB_CH, SUB_CH)
        large.append(pltpu.make_async_copy(spectra_hbm.at[part], spectra_ref.at[part], sems.at[band]))
    small[0].start()
    for copy in large:
        copy.start()
    for copy in small[1:]:
        copy.start()

    small[0].wait()
    lane = lax.broadcasted_iota(jnp.int32, (NDELAY, channels), 1)
    for band in range(bands):
        tiled = jnp.where(lane // SUB_CH == band, delay_ref[...], 0)
        step = SUB_CH
        while step < channels:
            tiled = tiled + pltpu.roll(tiled, step, 1)
            step *= 2
        for coarse in range(COARSE):
            for start in range(0, FINE, bands):
                wanted = coarse * FINE + start + lane // SUB_CH
                table = jnp.where(tiled == wanted, 1.0, 0.0).astype(jnp.bfloat16)
                tables_ref[band, coarse * NDELAY : (coarse + 1) * NDELAY, start * SUB_CH : start * SUB_CH + channels] = table

    def fill(band, fine):
        slot = band % 2
        for start in range(0, SUB_CH, HALF):
            at = fine * SUB_CH + start
            if fine == 0:
                first = spectra_ref[band * SUB_CH + start : band * SUB_CH + start + HALF, :]
                high = first.astype(jnp.bfloat16)
                low = (first - high.astype(jnp.float32)).astype(jnp.bfloat16)
            else:
                high = later(terms_ref[slot, start : start + HALF, :], fine)
                low = later(terms_ref[slot, depth + start : depth + start + HALF, :], fine)
            terms_ref[slot, at : at + HALF, :] = high
            terms_ref[slot, depth + at : depth + at + HALF, :] = low

    def multiply(band, tile):
        slot = band % 2
        table = tables_ref[band]
        both = jnp.concatenate([table, table], axis=1)
        columns = slice(tile * TILE, (tile + 1) * TILE)
        sums_ref[slot, :, columns] = jnp.dot(both, terms_ref[slot, :, columns], preferred_element_type=jnp.float32)

    def drain(band, start):
        slot = band % 2
        total = sums_ref[slot, start : start + HALF, :]
        for coarse in range(1, COARSE):
            at = coarse * NDELAY + start
            total = total + later(sums_ref[slot, at : at + HALF, :], coarse * FINE)
        rows_ref[band * NDELAY + start : band * NDELAY + start + HALF, :] = (total * SUB_CH ** (-0.5)).astype(jnp.bfloat16)

    tiles = samples // TILE
    for step in range(bands + 2):
        if step < bands:
            large[step].wait()
        for tile in range(tiles):
            if step < bands:
                for fine in range(tile * FINE // tiles, (tile + 1) * FINE // tiles):
                    fill(step, fine)
            if 1 <= step <= bands:
                multiply(step - 1, tile)
            if step >= 2:
                for start in range(0, NDELAY, HALF):
                    if (start // HALF + 1) * tiles // (NDELAY // HALF) - 1 == tile:
                        drain(step - 2, start)
        if step == 0:
            small[1].wait()
            base_of = jnp.transpose(base_ref[...])
            lane = lax.broadcasted_iota(jnp.int32, (owners, width), 1)
            base = jnp.zeros((owners, width), jnp.int32)
            for band in range(bands):
                base = jnp.where(lane // NDELAY == band, base_of[:, band : band + 1], base)
            lane = lax.broadcasted_iota(jnp.int32, (count, width), 1)
            place = lax.broadcasted_iota(jnp.int32, (count, width), 0)
            within = jnp.where(place // SPAN == lane // NDELAY, lane % NDELAY - place % SPAN, -1)
            for owner in range(owners):
                pick = jnp.where(base[owner : owner + 1, :] == within, 1.0, 0.0)
                picks_ref[owner * count : (owner + 1) * count, :] = pick.astype(jnp.bfloat16)
        if step == 1:
            small[2].wait()
            small[3].wait()
            small[4].wait()
            subbands = offset_in.shape[1]
            spread = lax.broadcasted_iota(jnp.int32, (subbands, subbands * SPAN), 1) // SPAN
            spread = (spread == lax.broadcasted_iota(jnp.int32, (subbands, subbands * SPAN), 0)).astype(jnp.bfloat16)
            wide = jnp.dot(offset_in[...].astype(jnp.bfloat16), spread, preferred_element_type=jnp.float32)
            span_of = (lax.broadcasted_iota(jnp.int32, wide.shape, 1) % SPAN).astype(jnp.float32)
            picker_ref[...] = jnp.where(wide == span_of, 1.0, 0.0).astype(jnp.bfloat16)
            shift_ref[...] = jnp.broadcast_to(column(shift_in[...], shift_ref.shape[0]), shift_ref.shape)
            length_ref[...] = jnp.broadcast_to(column(length_in[...], length_ref.shape[0]), length_ref.shape)

    total = owners * count
    group = min(total, TILE)
    for start in range(0, total, group):
        for tile in range(tiles):
            columns = slice(tile * TILE, (tile + 1) * TILE)
            picked = jnp.dot(picks_ref[start : start + group, :], rows_ref[:, columns], preferred_element_type=jnp.float32)
            windows_ref[start : start + group, columns] = picked.astype(jnp.bfloat16)


def scores_kernel(stacked_ref, picker_ref, shift_ref, length_ref, out_hbm, prefix_ref, after_ref, out_ref, sems):
    trials, templates, samples = out_ref.shape
    blocks = samples // BLOCK
    subbands = picker_ref.shape[1] // SPAN
    summed = jnp.dot(picker_ref[...], stacked_ref[...], preferred_element_type=jnp.float32) * subbands ** (-0.5)
    current = [summed[:, b * BLOCK : (b + 1) * BLOCK] for b in range(blocks)]
    shift = shift_ref[...]
    bit = 1
    while bit < blocks:
        taken = (shift & bit) != 0
        current = [jnp.where(taken, current[b + bit] if b + bit < blocks else 0.0, current[b]) for b in range(blocks)]
        bit *= 2
    whole = jnp.concatenate(current, axis=0)
    high = whole.astype(jnp.bfloat16)
    rest = whole - high.astype(jnp.float32)
    middle = rest.astype(jnp.bfloat16)
    low = (rest - middle.astype(jnp.float32)).astype(jnp.bfloat16)
    row = lax.broadcasted_iota(jnp.int32, (BLOCK, 2 * BLOCK), 0)
    lane = lax.broadcasted_iota(jnp.int32, (BLOCK, 2 * BLOCK), 1)
    ones = jnp.where((row < lane) | (lane >= BLOCK), 1.0, 0.0).astype(jnp.bfloat16)
    both = jnp.dot(
        jnp.concatenate([high, middle, low], axis=1), jnp.concatenate([ones, ones, ones], axis=0), preferred_element_type=jnp.float32
    )
    for b in range(blocks):
        columns = slice(b * BLOCK, (b + 1) * BLOCK)
        prefix_ref[:, columns] = both[b * trials : (b + 1) * trials, :BLOCK]
        after = both[b * trials : (b + 1) * trials, BLOCK:]
        if b + 1 < blocks:
            after = after + both[(b + 1) * trials : (b + 2) * trials, :BLOCK]
        after_ref[:, columns] = after
    length = length_ref[...]
    lane = lax.broadcasted_iota(jnp.int32, (templates, BLOCK), 1)
    source = (lane + length) % BLOCK
    from_next = lane < length
    weight = lax.rsqrt(length.astype(jnp.float32))
    chunk = trials // sems.shape[0]
    copies = []
    for j in range(trials):
        for b in range(blocks):
            columns = slice(b * BLOCK, (b + 1) * BLOCK)
            here = jnp.broadcast_to(prefix_ref[j : j + 1, columns], (templates, BLOCK))
            there = jnp.broadcast_to(after_ref[j : j + 1, columns], (templates, BLOCK))
            ends = jnp.take_along_axis(jnp.where(from_next, there, here), source, axis=1)
            out_ref[j, :, columns] = (ends - here) * weight
        if (j + 1) % chunk == 0:
            part = pl.ds(j + 1 - chunk, chunk)
            copies.append(pltpu.make_async_copy(out_ref.at[part], out_hbm.at[part], sems.at[len(copies)]))
            copies[-1].start()
    for copy in copies:
        copy.wait()


def local(spectra, chan_delay, window_base, trial_offset, shift_blocks, template_len):
    channels, samples = spectra.shape
    owners = window_base.shape[0]
    bands = channels // SUB_CH
    trials, subbands = trial_offset.shape
    templates = template_len.shape[0]
    count = bands * SPAN
    depth = FINE * SUB_CH
    anywhere = pl.BlockSpec(memory_space=pltpu.HBM)
    inside = pl.BlockSpec(memory_space=pltpu.VMEM)
    limits = pltpu.CompilerParams(vmem_limit_bytes=24 * 1024 * 1024)
    arrays = (spectra, chan_delay.T, window_base.T, trial_offset, shift_blocks.reshape(1, trials), template_len.reshape(1, templates))
    windows, picker, shift, length = pl.pallas_call(
        rows_kernel,
        out_shape=(
            pltpu.VMEM((owners * count, samples), jnp.bfloat16),
            pltpu.VMEM((trials, subbands * SPAN), jnp.bfloat16),
            pltpu.VMEM((trials, BLOCK), jnp.int32),
            pltpu.VMEM((templates, BLOCK), jnp.int32),
        ),
        in_specs=[anywhere] * 6,
        scratch_shapes=[
            pltpu.VMEM((channels, samples), jnp.float32),
            pltpu.VMEM((NDELAY, channels), jnp.int32),
            pltpu.VMEM((bands, owners), jnp.int32),
            pltpu.VMEM((trials, subbands), jnp.int32),
            pltpu.VMEM((1, trials), jnp.int32),
            pltpu.VMEM((1, templates), jnp.int32),
            pltpu.VMEM((bands, COARSE * NDELAY, depth), jnp.bfloat16),
            pltpu.VMEM((owners * count, bands * NDELAY), jnp.bfloat16),
            pltpu.VMEM((2, 2 * depth, samples), jnp.bfloat16),
            pltpu.VMEM((2, COARSE * NDELAY, samples), jnp.float32),
            pltpu.VMEM((bands * NDELAY, samples), jnp.bfloat16),
            pltpu.SemaphoreType.DMA((bands + 5,)),
        ],
        compiler_params=limits,
        name="rows",
    )(*(pltpu.with_memory_space_constraint(array, pltpu.HBM) for array in arrays))
    stacked = lax.all_to_all(windows, "chan", split_axis=0, concat_axis=0, tiled=True)
    stacked = pltpu.with_memory_space_constraint(stacked, pltpu.VMEM)
    return pl.pallas_call(
        scores_kernel,
        out_shape=jax.ShapeDtypeStruct((trials, templates, samples), jnp.float32),
        in_specs=[inside] * 4,
        out_specs=anywhere,
        scratch_shapes=[
            pltpu.VMEM((trials, samples), jnp.float32),
            pltpu.VMEM((trials, samples), jnp.float32),
            pltpu.VMEM((trials, templates, samples), jnp.float32),
            pltpu.SemaphoreType.DMA((4,)),
        ],
        compiler_params=limits,
        name="scores",
    )(stacked, picker, shift, length)


def solution(mesh):
    in_specs = (
        P(("beam", "chan"), None),
        P("chan", None),
        P(None, "chan"),
        P("chan", None),
        P("chan"),
        P(),
    )
    out_specs = P(("beam", "chan"), None, None)
    return jax.shard_map(local, mesh=mesh, in_specs=in_specs, out_specs=out_specs, check_vma=False)
```

```python
import jax
import jax.numpy as jnp
from jax import lax
from jax.experimental import pallas as pl
from jax.experimental.pallas import tpu as pltpu
from jax.sharding import PartitionSpec as P

SUB_CH = 32
NDELAY = 32
MAXD = 64
SPAN = 4
BLOCK = 128
FINE = 8
COARSE = MAXD // FINE
TILE = 256
HALF = 16
CORES = 2
ORDER = (4, 7, 1, 6, 3, 5, 2)


def later(x, amount):
    if amount == 0:
        return x
    moved = pltpu.roll(x, amount, 1)
    lane = lax.broadcasted_iota(jnp.int32, (x.shape[0], BLOCK), 1)
    first = jnp.where(lane >= amount, moved[:, :BLOCK], jnp.zeros((), x.dtype))
    return jnp.concatenate([first, moved[:, BLOCK:]], axis=1)


def partner(chip, distance):
    return chip ^ distance


def column(row, size):
    same = lax.broadcasted_iota(jnp.int32, (size, size), 0) == lax.broadcasted_iota(jnp.int32, (size, size), 1)
    return jnp.sum(jnp.where(same, row.astype(jnp.float32), 0.0), axis=1, keepdims=True).astype(jnp.int32)


def rows_kernel(
    spectra_hbm, delay_hbm, base_hbm, offset_hbm, shift_hbm, length_hbm,
    keep_ref, give_ref, picker_ref, shift_ref, length_ref,
    spectra_ref, delay_ref, base_ref, offset_in, shift_in, length_in,
    tables_ref, picks_ref, lanes_ref, terms_ref, sums_ref, rows_ref, sems,
):
    me = lax.axis_index("chan")
    chip, core = me // CORES, me % CORES
    channels, samples = spectra_ref.shape
    bands = channels // SUB_CH
    owners = base_ref.shape[1]
    depth = FINE * SUB_CH
    width = bands * NDELAY
    count = bands * SPAN
    chips = owners // CORES

    small = [
        pltpu.make_async_copy(source, target, sems.at[bands + i])
        for i, (source, target) in enumerate(
            [(delay_hbm, delay_ref), (base_hbm, base_ref), (offset_hbm, offset_in), (shift_hbm, shift_in), (length_hbm, length_in)]
        )
    ]
    large = []
    for band in range(bands):
        part = pl.ds(band * SUB_CH, SUB_CH)
        large.append(pltpu.make_async_copy(spectra_hbm.at[part], spectra_ref.at[part], sems.at[band]))
    small[0].start()
    for copy in large:
        copy.start()
    for copy in small[1:]:
        copy.start()

    small[0].wait()
    lane = lax.broadcasted_iota(jnp.int32, (NDELAY, channels), 1)
    for band in range(bands):
        tiled = jnp.where(lane // SUB_CH == band, delay_ref[...], 0)
        step = SUB_CH
        while step < channels:
            tiled = tiled + pltpu.roll(tiled, step, 1)
            step *= 2
        for coarse in range(COARSE):
            for start in range(0, FINE, bands):
                wanted = coarse * FINE + start + lane // SUB_CH
                table = jnp.where(tiled == wanted, 1.0, 0.0).astype(jnp.bfloat16)
                tables_ref[band, coarse * NDELAY : (coarse + 1) * NDELAY, start * SUB_CH : start * SUB_CH + channels] = table

    def fill(band, fine):
        slot = band % 2
        for start in range(0, SUB_CH, HALF):
            at = fine * SUB_CH + start
            if fine == 0:
                first = spectra_ref[band * SUB_CH + start : band * SUB_CH + start + HALF, :]
                high = first.astype(jnp.bfloat16)
                low = (first - high.astype(jnp.float32)).astype(jnp.bfloat16)
            else:
                high = later(terms_ref[slot, start : start + HALF, :], fine)
                low = later(terms_ref[slot, depth + start : depth + start + HALF, :], fine)
            terms_ref[slot, at : at + HALF, :] = high
            terms_ref[slot, depth + at : depth + at + HALF, :] = low

    def multiply(band, tile):
        slot = band % 2
        table = tables_ref[band]
        both = jnp.concatenate([table, table], axis=1)
        columns = slice(tile * TILE, (tile + 1) * TILE)
        sums_ref[slot, :, columns] = jnp.dot(both, terms_ref[slot, :, columns], preferred_element_type=jnp.float32)

    def drain(band, start):
        slot = band % 2
        total = sums_ref[slot, start : start + HALF, :]
        for coarse in range(1, COARSE):
            at = coarse * NDELAY + start
            total = total + later(sums_ref[slot, at : at + HALF, :], coarse * FINE)
        rows_ref[band * NDELAY + start : band * NDELAY + start + HALF, :] = (total * SUB_CH ** (-0.5)).astype(jnp.bfloat16)

    tiles = samples // TILE
    for step in range(bands + 2):
        if step < bands:
            large[step].wait()
        for tile in range(tiles):
            if step < bands:
                for fine in range(tile * FINE // tiles, (tile + 1) * FINE // tiles):
                    fill(step, fine)
            if 1 <= step <= bands:
                multiply(step - 1, tile)
            if step >= 2:
                for start in range(0, NDELAY, HALF):
                    if (start // HALF + 1) * tiles // (NDELAY // HALF) - 1 == tile:
                        drain(step - 2, start)
        if step == 0:
            small[1].wait()
            base_of = jnp.transpose(base_ref[...])
            lane = lax.broadcasted_iota(jnp.int32, (owners, width), 1)
            base = jnp.zeros((owners, width), jnp.int32)
            for band in range(bands):
                base = jnp.where(lane // NDELAY == band, base_of[:, band : band + 1], base)
            lane = lax.broadcasted_iota(jnp.int32, (count, width), 1)
            place = lax.broadcasted_iota(jnp.int32, (count, width), 0)
            within = jnp.where(place // SPAN == lane // NDELAY, lane % NDELAY - place % SPAN, -1)
            lanes_ref[...] = base
            for place_of in range(owners):
                side, distance = place_of // chips, place_of % chips
                owner = partner(chip, distance) * CORES + (core + side) % CORES
                pick = jnp.where(lanes_ref[pl.ds(owner, 1), :] == within, 1.0, 0.0)
                picks_ref[place_of * count : (place_of + 1) * count, :] = pick.astype(jnp.bfloat16)
        if step == 1:
            small[2].wait()
            small[3].wait()
            small[4].wait()
            subbands = offset_in.shape[1]
            place = lax.broadcasted_iota(jnp.int32, (subbands, subbands * SPAN), 1) // SPAN
            side = place // bands % CORES
            spread = (partner(chip, place // (bands * CORES)) * CORES + (core + side) % CORES) * bands + place % bands
            spread = (spread == lax.broadcasted_iota(jnp.int32, (subbands, subbands * SPAN), 0)).astype(jnp.bfloat16)
            wide = jnp.dot(offset_in[...].astype(jnp.bfloat16), spread, preferred_element_type=jnp.float32)
            span_of = (lax.broadcasted_iota(jnp.int32, wide.shape, 1) % SPAN).astype(jnp.float32)
            picker_ref[...] = jnp.where(wide == span_of, 1.0, 0.0).astype(jnp.bfloat16)
            shift_ref[...] = jnp.broadcast_to(column(shift_in[...], shift_ref.shape[0]), shift_ref.shape)
            length_ref[...] = jnp.broadcast_to(column(length_in[...], length_ref.shape[0]), length_ref.shape)

    total = chips * count
    group = min(total, TILE)
    for side, target in enumerate((keep_ref, give_ref)):
        for start in range(0, total, group):
            for tile in range(tiles):
                columns = slice(tile * TILE, (tile + 1) * TILE)
                part = slice(side * total + start, side * total + start + group)
                picked = jnp.dot(picks_ref[part, :], rows_ref[:, columns], preferred_element_type=jnp.float32)
                target[start : start + group, columns] = picked.astype(jnp.bfloat16)


def join_kernel(keep_ref, got_ref, *parts):
    count = parts[0].shape[0] // CORES
    for distance, part in zip(order(len(parts) + 1), parts):
        rows = slice(distance * count, (distance + 1) * count)
        part[:count, :] = keep_ref[rows, :]
        part[count:, :] = got_ref[rows, :]


def scores_kernel(keep_ref, got_ref, picker_ref, shift_ref, length_ref, *rest):
    *parts, out_hbm, prefix_ref, after_ref, out_ref, sems = rest
    trials, templates, samples = out_ref.shape
    blocks = samples // BLOCK
    subbands = picker_ref.shape[1] // SPAN
    count = parts[0].shape[0] // CORES
    near = dict(zip(order(len(parts) + 1), parts))
    stacked = [keep_ref[:count, :], got_ref[:count, :]] + [near[distance][...] for distance in sorted(near)]
    stacked = jnp.concatenate(stacked, axis=0)
    summed = jnp.dot(picker_ref[...], stacked, preferred_element_type=jnp.float32) * subbands ** (-0.5)
    current = [summed[:, b * BLOCK : (b + 1) * BLOCK] for b in range(blocks)]
    shift = shift_ref[...]
    bit = 1
    while bit < blocks:
        taken = (shift & bit) != 0
        current = [jnp.where(taken, current[b + bit] if b + bit < blocks else 0.0, current[b]) for b in range(blocks)]
        bit *= 2
    whole = jnp.concatenate(current, axis=0)
    high = whole.astype(jnp.bfloat16)
    rest = whole - high.astype(jnp.float32)
    middle = rest.astype(jnp.bfloat16)
    low = (rest - middle.astype(jnp.float32)).astype(jnp.bfloat16)
    row = lax.broadcasted_iota(jnp.int32, (BLOCK, 2 * BLOCK), 0)
    lane = lax.broadcasted_iota(jnp.int32, (BLOCK, 2 * BLOCK), 1)
    ones = jnp.where((row < lane) | (lane >= BLOCK), 1.0, 0.0).astype(jnp.bfloat16)
    both = jnp.dot(
        jnp.concatenate([high, middle, low], axis=1), jnp.concatenate([ones, ones, ones], axis=0), preferred_element_type=jnp.float32
    )
    for b in range(blocks):
        columns = slice(b * BLOCK, (b + 1) * BLOCK)
        prefix_ref[:, columns] = both[b * trials : (b + 1) * trials, :BLOCK]
        after = both[b * trials : (b + 1) * trials, BLOCK:]
        if b + 1 < blocks:
            after = after + both[(b + 1) * trials : (b + 2) * trials, :BLOCK]
        after_ref[:, columns] = after
    length = length_ref[...]
    lane = lax.broadcasted_iota(jnp.int32, (templates, BLOCK), 1)
    source = (lane + length) % BLOCK
    from_next = lane < length
    weight = lax.rsqrt(length.astype(jnp.float32))
    chunk = trials // sems.shape[0]
    copies = []
    for j in range(trials):
        for b in range(blocks):
            columns = slice(b * BLOCK, (b + 1) * BLOCK)
            here = jnp.broadcast_to(prefix_ref[j : j + 1, columns], (templates, BLOCK))
            there = jnp.broadcast_to(after_ref[j : j + 1, columns], (templates, BLOCK))
            ends = jnp.take_along_axis(jnp.where(from_next, there, here), source, axis=1)
            out_ref[j, :, columns] = (ends - here) * weight
        if (j + 1) % chunk == 0:
            part = pl.ds(j + 1 - chunk, chunk)
            copies.append(pltpu.make_async_copy(out_ref.at[part], out_hbm.at[part], sems.at[len(copies)]))
            copies[-1].start()
    for copy in copies:
        copy.wait()


def order(chips):
    if chips == len(ORDER) + 1:
        return ORDER
    return range(1, chips)


def local(spectra, chan_delay, window_base, trial_offset, shift_blocks, template_len):
    channels, samples = spectra.shape
    owners = window_base.shape[0]
    bands = channels // SUB_CH
    trials, subbands = trial_offset.shape
    templates = template_len.shape[0]
    count = bands * SPAN
    chips = owners // CORES
    depth = FINE * SUB_CH
    anywhere = pl.BlockSpec(memory_space=pltpu.HBM)
    inside = pl.BlockSpec(memory_space=pltpu.VMEM)
    limits = pltpu.CompilerParams(vmem_limit_bytes=24 * 1024 * 1024)
    arrays = (spectra, chan_delay.T, window_base.T, trial_offset, shift_blocks.reshape(1, trials), template_len.reshape(1, templates))
    keep, give, picker, shift, length = pl.pallas_call(
        rows_kernel,
        out_shape=(
            pltpu.VMEM((chips * count, samples), jnp.bfloat16),
            pltpu.VMEM((chips * count, samples), jnp.bfloat16),
            pltpu.VMEM((trials, subbands * SPAN), jnp.bfloat16),
            pltpu.VMEM((trials, BLOCK), jnp.int32),
            pltpu.VMEM((templates, BLOCK), jnp.int32),
        ),
        in_specs=[anywhere] * 6,
        scratch_shapes=[
            pltpu.VMEM((channels, samples), jnp.float32),
            pltpu.VMEM((NDELAY, channels), jnp.int32),
            pltpu.VMEM((bands, owners), jnp.int32),
            pltpu.VMEM((trials, subbands), jnp.int32),
            pltpu.VMEM((1, trials), jnp.int32),
            pltpu.VMEM((1, templates), jnp.int32),
            pltpu.VMEM((bands, COARSE * NDELAY, depth), jnp.bfloat16),
            pltpu.VMEM((owners * count, bands * NDELAY), jnp.bfloat16),
            pltpu.VMEM((owners, bands * NDELAY), jnp.int32),
            pltpu.VMEM((2, 2 * depth, samples), jnp.bfloat16),
            pltpu.VMEM((2, COARSE * NDELAY, samples), jnp.float32),
            pltpu.VMEM((bands * NDELAY, samples), jnp.bfloat16),
            pltpu.SemaphoreType.DMA((bands + 5,)),
        ],
        compiler_params=limits,
        name="rows",
    )(*(pltpu.with_memory_space_constraint(array, pltpu.HBM) for array in arrays))
    devices = range(owners)
    got = lax.ppermute(give, "chan", [(i, i ^ 1) for i in devices])
    got = pltpu.with_memory_space_constraint(got, pltpu.VMEM)
    parts = pl.pallas_call(
        join_kernel,
        out_shape=[pltpu.VMEM((CORES * count, samples), jnp.bfloat16)] * (chips - 1),
        in_specs=[inside] * 2,
        compiler_params=limits,
        name="join",
    )(keep, got)
    arrived = []
    for distance, part in zip(order(chips), parts):
        part = lax.ppermute(part, "chan", [(i, partner(i // CORES, distance) * CORES + i % CORES) for i in devices])
        arrived.append(pltpu.with_memory_space_constraint(part, pltpu.VMEM))
    return pl.pallas_call(
        scores_kernel,
        out_shape=jax.ShapeDtypeStruct((trials, templates, samples), jnp.float32),
        in_specs=[inside] * (5 + len(arrived)),
        out_specs=anywhere,
        scratch_shapes=[
            pltpu.VMEM((trials, samples), jnp.float32),
            pltpu.VMEM((trials, samples), jnp.float32),
            pltpu.VMEM((trials, templates, samples), jnp.float32),
            pltpu.SemaphoreType.DMA((4,)),
        ],
        compiler_params=limits,
        name="scores",
    )(keep, got, picker, shift, length, *arrived)


def solution(mesh):
    in_specs = (
        P(("beam", "chan"), None),
        P("chan", None),
        P(None, "chan"),
        P("chan", None),
        P("chan"),
        P(),
    )
    out_specs = P(("beam", "chan"), None, None)
    return jax.shard_map(local, mesh=mesh, in_specs=in_specs, out_specs=out_specs, check_vma=False)
```

```python
import functools

import jax
import jax.numpy as jnp
from jax import lax
from jax.experimental import pallas as pl
from jax.experimental.pallas import tpu as pltpu
from jax.sharding import PartitionSpec as P


SUB_CH = 32
NDELAY = 32
MAXD = 64
SPAN = 4
BLOCK = 128
FINE = 8
COARSE = MAXD // FINE
TILE = 256
HALF = 16
CORES = 2
ORDER = (4, 5, 3, 6, 7, 2, 1)


def later(x, amount):
    if amount == 0:
        return x
    moved = pltpu.roll(x, amount, 1)
    lane = lax.broadcasted_iota(jnp.int32, (x.shape[0], BLOCK), 1)
    first = jnp.where(lane >= amount, moved[:, :BLOCK], jnp.zeros((), x.dtype))
    return jnp.concatenate([first, moved[:, BLOCK:]], axis=1)


def partner(chip, distance):
    return chip ^ distance


def column(row, size):
    same = lax.broadcasted_iota(jnp.int32, (size, size), 0) == lax.broadcasted_iota(jnp.int32, (size, size), 1)
    return jnp.sum(jnp.where(same, row.astype(jnp.float32), 0.0), axis=1, keepdims=True).astype(jnp.int32)


def rows_kernel(
    spectra_hbm, delay_hbm, base_hbm, keep_ref, give_ref,
    spectra_ref, delay_ref, base_ref, tables_ref, terms_ref, sums_ref, rows_ref, sems,
):
    me = lax.axis_index("chan")
    chip, core = me // CORES, me % CORES
    channels, samples = spectra_ref.shape
    bands = channels // SUB_CH
    owners = base_ref.shape[1]
    depth = FINE * SUB_CH
    count = bands * SPAN
    chips = owners // CORES
    blocks = samples // BLOCK

    large = []
    for band in range(bands):
        part = pl.ds(band * SUB_CH, SUB_CH)
        large.append(pltpu.make_async_copy(spectra_hbm.at[part], spectra_ref.at[part], sems.at[band]))
    delays = pltpu.make_async_copy(delay_hbm, delay_ref, sems.at[bands])
    bases = pltpu.make_async_copy(base_hbm, base_ref, sems.at[bands + 1])
    large[0].start()
    delays.start()
    for copy in large[1:]:
        copy.start()
    bases.start()
    rows_ref[:, bands * NDELAY :, :] = jnp.zeros((blocks, rows_ref.shape[1] - bands * NDELAY, BLOCK), jnp.float32)

    def tabulate(band):
        lane = lax.broadcasted_iota(jnp.int32, (NDELAY, channels), 1)
        tiled = jnp.where(lane // SUB_CH == band, delay_ref[...], 0)
        step = SUB_CH
        while step < channels:
            tiled = tiled + pltpu.roll(tiled, step, 1)
            step *= 2
        for coarse in range(COARSE):
            for start in range(0, FINE, bands):
                wanted = coarse * FINE + start + lane // SUB_CH
                table = jnp.where(tiled == wanted, 1.0, 0.0).astype(jnp.bfloat16)
                tables_ref[band, coarse * NDELAY : (coarse + 1) * NDELAY, start * SUB_CH : start * SUB_CH + channels] = table

    def fill(band, fine):
        slot = band % 2
        for start in range(0, SUB_CH, HALF):
            at = fine * SUB_CH + start
            if fine == 0:
                first = spectra_ref[band * SUB_CH + start : band * SUB_CH + start + HALF, :]
                high = first.astype(jnp.bfloat16)
                low = (first - high.astype(jnp.float32)).astype(jnp.bfloat16)
            else:
                high = later(terms_ref[slot, start : start + HALF, :], fine)
                low = later(terms_ref[slot, depth + start : depth + start + HALF, :], fine)
            terms_ref[slot, at : at + HALF, :] = high
            terms_ref[slot, depth + at : depth + at + HALF, :] = low

    def multiply(band, tile):
        slot = band % 2
        table = tables_ref[band]
        both = jnp.concatenate([table, table], axis=1)
        columns = slice(tile * TILE, (tile + 1) * TILE)
        sums_ref[slot, :, columns] = jnp.dot(both, terms_ref[slot, :, columns], preferred_element_type=jnp.float32)

    def drain(band, start):
        slot = band % 2
        total = sums_ref[slot, start : start + HALF, :]
        for coarse in range(1, COARSE):
            at = coarse * NDELAY + start
            total = total + later(sums_ref[slot, at : at + HALF, :], coarse * FINE)
        total = total * SUB_CH ** (-0.5)
        for block in range(blocks):
            at = band * NDELAY + start
            rows_ref[block, at : at + HALF, :] = total[:, block * BLOCK : (block + 1) * BLOCK]

    tiles = samples // TILE
    for step in range(bands + 2):
        if step < bands:
            large[step].wait()
        for tile in range(tiles):
            if step < bands:
                for fine in range(tile * FINE // tiles, (tile + 1) * FINE // tiles):
                    fill(step, fine)
            if 1 <= step <= bands:
                multiply(step - 1, tile)
            if step >= 2:
                for start in range(0, NDELAY, HALF):
                    if (start // HALF + 1) * tiles // (NDELAY // HALF) - 1 == tile:
                        drain(step - 2, start)
        if step < bands:
            if step == 0:
                delays.wait()
            tabulate(step)

    bases.wait()
    place = lax.broadcasted_iota(jnp.int32, (2 * SPAN, BLOCK), 0)
    for side, target in ((1, give_ref), (0, keep_ref)):
        for distance in range(chips):
            owner = partner(chip, distance) * CORES + (core + side) % CORES
            begins = [band * NDELAY + base_ref[band, owner] for band in range(bands)]
            for block in range(blocks):
                pairs = []
                for band in range(0, bands, 2):
                    upper = rows_ref[block, pl.ds(begins[band], 2 * SPAN), :]
                    lower = rows_ref[block, pl.ds(begins[band + 1] - SPAN, 2 * SPAN), :]
                    pairs.append(jnp.where(place < SPAN, upper, lower))
                picked = jnp.concatenate(pairs, axis=0).astype(jnp.bfloat16)
                target[distance * count : (distance + 1) * count, block * BLOCK : (block + 1) * BLOCK] = picked


def tables_kernel(offset_ref, shift_in, length_in, picker_ref, shift_ref, length_ref, ones_ref, *, bands):
    me = lax.axis_index("chan")
    chip, core = me // CORES, me % CORES
    subbands = offset_ref.shape[1]
    place = lax.broadcasted_iota(jnp.int32, (subbands, subbands * SPAN), 1) // SPAN
    side = place // bands % CORES
    spread = (partner(chip, place // (bands * CORES)) * CORES + (core + side) % CORES) * bands + place % bands
    spread = (spread == lax.broadcasted_iota(jnp.int32, (subbands, subbands * SPAN), 0)).astype(jnp.bfloat16)
    wide = jnp.dot(offset_ref[...].astype(jnp.bfloat16), spread, preferred_element_type=jnp.float32)
    span_of = (lax.broadcasted_iota(jnp.int32, wide.shape, 1) % SPAN).astype(jnp.float32)
    picker_ref[...] = jnp.where(wide == span_of, 1.0, 0.0).astype(jnp.bfloat16)
    shift_ref[...] = jnp.broadcast_to(column(shift_in[...], shift_ref.shape[0]), shift_ref.shape)
    length_ref[...] = jnp.broadcast_to(column(length_in[...], length_ref.shape[0]), length_ref.shape)
    row = lax.broadcasted_iota(jnp.int32, ones_ref.shape, 0) % BLOCK
    lane = lax.broadcasted_iota(jnp.int32, ones_ref.shape, 1)
    ones_ref[...] = jnp.where((row < lane) | (lane >= BLOCK), 1.0, 0.0).astype(jnp.bfloat16)


def join_kernel(keep_ref, got_ref, *parts):
    count = parts[0].shape[0] // CORES
    for distance, part in zip(order(len(parts) + 1), parts):
        rows = slice(distance * count, (distance + 1) * count)
        part[:count, :] = keep_ref[rows, :]
        part[count:, :] = got_ref[rows, :]


def scores_kernel(keep_ref, got_ref, picker_ref, shift_ref, length_ref, ones_ref, *rest):
    *parts, out_hbm, prefix_ref, after_ref, out_ref, sems = rest
    trials, templates, samples = out_ref.shape
    blocks = samples // BLOCK
    subbands = picker_ref.shape[1] // SPAN
    count = parts[0].shape[0] // CORES
    near = dict(zip(order(len(parts) + 1), parts))
    stacked = [keep_ref[:count, :], got_ref[:count, :]] + [near[distance][...] for distance in sorted(near)]
    stacked = jnp.concatenate(stacked, axis=0)
    summed = jnp.dot(picker_ref[...], stacked, preferred_element_type=jnp.float32) * subbands ** (-0.5)
    current = [summed[:, b * BLOCK : (b + 1) * BLOCK] for b in range(blocks)]
    shift = shift_ref[...]
    bit = 1
    while bit < blocks:
        taken = (shift & bit) != 0
        current = [jnp.where(taken, current[b + bit] if b + bit < blocks else 0.0, current[b]) for b in range(blocks)]
        bit *= 2
    whole = jnp.concatenate(current, axis=0)
    high = whole.astype(jnp.bfloat16)
    rest = whole - high.astype(jnp.float32)
    middle = rest.astype(jnp.bfloat16)
    low = (rest - middle.astype(jnp.float32)).astype(jnp.bfloat16)
    both = jnp.dot(jnp.concatenate([high, middle, low], axis=1), ones_ref[...], preferred_element_type=jnp.float32)
    for b in range(blocks):
        columns = slice(b * BLOCK, (b + 1) * BLOCK)
        prefix_ref[:, columns] = both[b * trials : (b + 1) * trials, :BLOCK]
        after = both[b * trials : (b + 1) * trials, BLOCK:]
        if b + 1 < blocks:
            after = after + both[(b + 1) * trials : (b + 2) * trials, :BLOCK]
        after_ref[:, columns] = after
    length = length_ref[...]
    lane = lax.broadcasted_iota(jnp.int32, (templates, BLOCK), 1)
    source = (lane + length) % BLOCK
    from_next = lane < length
    weight = lax.rsqrt(length.astype(jnp.float32))
    chunk = trials // sems.shape[0]
    copies = []
    for j in range(trials):
        for b in range(blocks):
            columns = slice(b * BLOCK, (b + 1) * BLOCK)
            here = jnp.broadcast_to(prefix_ref[j : j + 1, columns], (templates, BLOCK))
            there = jnp.broadcast_to(after_ref[j : j + 1, columns], (templates, BLOCK))
            ends = jnp.take_along_axis(jnp.where(from_next, there, here), source, axis=1)
            out_ref[j, :, columns] = (ends - here) * weight
        if (j + 1) % chunk == 0:
            part = pl.ds(j + 1 - chunk, chunk)
            copies.append(pltpu.make_async_copy(out_ref.at[part], out_hbm.at[part], sems.at[len(copies)]))
            copies[-1].start()
    for copy in copies:
        copy.wait()


def order(chips):
    if chips == len(ORDER) + 1:
        return ORDER
    return tuple(range(1, chips))


def local(spectra, chan_delay, window_base, trial_offset, shift_blocks, template_len):
    channels, samples = spectra.shape
    owners = window_base.shape[0]
    bands = channels // SUB_CH
    trials, subbands = trial_offset.shape
    templates = template_len.shape[0]
    count = bands * SPAN
    chips = owners // CORES
    depth = FINE * SUB_CH
    anywhere = pl.BlockSpec(memory_space=pltpu.HBM)
    inside = pl.BlockSpec(memory_space=pltpu.VMEM)
    limits = pltpu.CompilerParams(vmem_limit_bytes=24 * 1024 * 1024)
    arrays = [
        pltpu.with_memory_space_constraint(array, pltpu.HBM)
        for array in (spectra, chan_delay.T, window_base.T, trial_offset, shift_blocks.reshape(1, trials), template_len.reshape(1, templates))
    ]
    keep, give = pl.pallas_call(
        rows_kernel,
        out_shape=[pltpu.VMEM((chips * count, samples), jnp.bfloat16)] * 2,
        in_specs=[anywhere] * 3,
        scratch_shapes=[
            pltpu.VMEM((channels, samples), jnp.float32),
            pltpu.VMEM((NDELAY, channels), jnp.int32),
            pltpu.SMEM((bands, owners), jnp.int32),
            pltpu.VMEM((bands, COARSE * NDELAY, depth), jnp.bfloat16),
            pltpu.VMEM((2, 2 * depth, samples), jnp.bfloat16),
            pltpu.VMEM((2, COARSE * NDELAY, samples), jnp.float32),
            pltpu.VMEM((samples // BLOCK, bands * NDELAY + 2 * SPAN, BLOCK), jnp.float32),
            pltpu.SemaphoreType.DMA((bands + 2,)),
        ],
        compiler_params=limits,
        name="rows",
    )(*arrays[:3])
    picker, shift, length, ones = pl.pallas_call(
        functools.partial(tables_kernel, bands=bands),
        out_shape=(
            pltpu.VMEM((trials, subbands * SPAN), jnp.bfloat16),
            pltpu.VMEM((trials, BLOCK), jnp.int32),
            pltpu.VMEM((templates, BLOCK), jnp.int32),
            pltpu.VMEM((3 * BLOCK, 2 * BLOCK), jnp.bfloat16),
        ),
        compiler_params=limits,
        name="tables",
    )(*arrays[3:])
    devices = range(owners)
    got = lax.ppermute(give, "chan", [(i, i ^ 1) for i in devices])
    got = pltpu.with_memory_space_constraint(got, pltpu.VMEM)
    parts = pl.pallas_call(
        join_kernel,
        out_shape=[pltpu.VMEM((CORES * count, samples), jnp.bfloat16)] * (chips - 1),
        in_specs=[inside] * 2,
        compiler_params=limits,
        name="join",
    )(keep, got)
    arrived = []
    for distance, part in zip(order(chips), parts):
        part = lax.ppermute(part, "chan", [(i, partner(i // CORES, distance) * CORES + i % CORES) for i in devices])
        arrived.append(pltpu.with_memory_space_constraint(part, pltpu.VMEM))
    return pl.pallas_call(
        scores_kernel,
        out_shape=jax.ShapeDtypeStruct((trials, templates, samples), jnp.float32),
        in_specs=[inside] * (6 + len(arrived)),
        out_specs=anywhere,
        scratch_shapes=[
            pltpu.VMEM((trials, samples), jnp.float32),
            pltpu.VMEM((trials, samples), jnp.float32),
            pltpu.VMEM((trials, templates, samples), jnp.float32),
            pltpu.SemaphoreType.DMA((4,)),
        ],
        compiler_params=limits,
        name="scores",
    )(keep, got, picker, shift, length, ones, *arrived)


def solution(mesh):
    in_specs = (
        P(("beam", "chan"), None),
        P("chan", None),
        P(None, "chan"),
        P("chan", None),
        P("chan"),
        P(),
    )
    out_specs = P(("beam", "chan"), None, None)

    return jax.shard_map(local, mesh=mesh, in_specs=in_specs, out_specs=out_specs, check_vma=False)
```

```python
import functools

import jax
import jax.numpy as jnp
from jax import lax
from jax.experimental import pallas as pl
from jax.experimental.pallas import tpu as pltpu
from jax.sharding import PartitionSpec as P


SUB_CH = 32
NDELAY = 32
MAXD = 64
SPAN = 4
BLOCK = 128
FINE = 8
COARSE = MAXD // FINE
PAIRED = 2
TILE = 256
HALF = 16
CORES = 2
ORDER = (4, 5, 3, 6, 7, 2, 1)


def later(x, amount):
    if amount == 0:
        return x
    moved = pltpu.roll(x, amount, 1)
    lane = lax.broadcasted_iota(jnp.int32, (x.shape[0], BLOCK), 1)
    first = jnp.where(lane >= amount, moved[:, :BLOCK], jnp.zeros((), x.dtype))
    return jnp.concatenate([first, moved[:, BLOCK:]], axis=1)


def partner(chip, distance):
    return chip ^ distance


def column(row, size):
    same = lax.broadcasted_iota(jnp.int32, (size, size), 0) == lax.broadcasted_iota(jnp.int32, (size, size), 1)
    return jnp.sum(jnp.where(same, row.astype(jnp.float32), 0.0), axis=1, keepdims=True).astype(jnp.int32)


def rows_kernel(
    spectra_hbm, delay_hbm, base_hbm, keep_ref, give_ref,
    spectra_ref, delay_ref, base_ref, moves_ref, tables_ref, terms_ref, sums_ref, rows_ref, sems,
):
    me = lax.axis_index("chan")
    chip, core = me // CORES, me % CORES
    channels, samples = spectra_ref.shape
    bands = channels // SUB_CH
    owners = base_ref.shape[1]
    depth = FINE * SUB_CH
    count = bands * SPAN
    chips = owners // CORES
    blocks = samples // BLOCK

    large = []
    for band in range(bands):
        part = pl.ds(band * SUB_CH, SUB_CH)
        large.append(pltpu.make_async_copy(spectra_hbm.at[part], spectra_ref.at[part], sems.at[band]))
    delays = pltpu.make_async_copy(delay_hbm, delay_ref, sems.at[bands])
    bases = pltpu.make_async_copy(base_hbm, base_ref, sems.at[bands + 1])
    delays.start()
    large[0].start()
    for copy in large[1:]:
        copy.start()
    bases.start()
    rows_ref[:, bands * NDELAY :, :] = jnp.zeros((blocks, rows_ref.shape[1] - bands * NDELAY, BLOCK), jnp.float32)

    row = lax.broadcasted_iota(jnp.int32, (2 * BLOCK, 2 * BLOCK), 0)
    lane = lax.broadcasted_iota(jnp.int32, (2 * BLOCK, 2 * BLOCK), 1)
    for pair in range(PAIRED // 2):
        fine = FINE - PAIRED + 2 * pair + lane // BLOCK
        move = jnp.where(row == BLOCK + lane % BLOCK - fine, 1.0, 0.0)
        moves_ref[:, pair * 2 * BLOCK : (pair + 1) * 2 * BLOCK] = move.astype(jnp.bfloat16)

    def move_pair(band, pair):
        slot = band % 2
        pieces = []
        for block in range(blocks):
            for start in (0, depth):
                now = terms_ref[slot, start : start + SUB_CH, block * BLOCK : (block + 1) * BLOCK]
                if block:
                    earlier = terms_ref[slot, start : start + SUB_CH, (block - 1) * BLOCK : block * BLOCK]
                else:
                    earlier = jnp.zeros_like(now)
                pieces.append(jnp.concatenate([earlier, now], axis=1))
        moved = jnp.dot(
            jnp.concatenate(pieces, axis=0), moves_ref[:, pair * 2 * BLOCK : (pair + 1) * 2 * BLOCK], preferred_element_type=jnp.float32
        ).astype(jnp.bfloat16)
        for block in range(blocks):
            for term, start in enumerate((0, depth)):
                rows = slice((2 * block + term) * SUB_CH, (2 * block + term + 1) * SUB_CH)
                for side in range(2):
                    at = start + (FINE - PAIRED + 2 * pair + side) * SUB_CH
                    piece = moved[rows, side * BLOCK : (side + 1) * BLOCK]
                    terms_ref[slot, at : at + SUB_CH, block * BLOCK : (block + 1) * BLOCK] = piece

    def tabulate(band):
        lane = lax.broadcasted_iota(jnp.int32, (NDELAY, channels), 1)
        tiled = jnp.where(lane // SUB_CH == band, delay_ref[...], 0)
        step = SUB_CH
        while step < channels:
            tiled = tiled + pltpu.roll(tiled, step, 1)
            step *= 2
        for coarse in range(COARSE):
            for start in range(0, FINE, bands):
                wanted = coarse * FINE + start + lane // SUB_CH
                table = jnp.where(tiled == wanted, 1.0, 0.0).astype(jnp.bfloat16)
                tables_ref[band, coarse * NDELAY : (coarse + 1) * NDELAY, start * SUB_CH : start * SUB_CH + channels] = table

    def fill(band, fine):
        slot = band % 2
        for start in range(0, SUB_CH, HALF):
            at = fine * SUB_CH + start
            if fine == 0:
                first = spectra_ref[band * SUB_CH + start : band * SUB_CH + start + HALF, :]
                high = first.astype(jnp.bfloat16)
                low = (first - high.astype(jnp.float32)).astype(jnp.bfloat16)
            else:
                high = later(terms_ref[slot, start : start + HALF, :], fine)
                low = later(terms_ref[slot, depth + start : depth + start + HALF, :], fine)
            terms_ref[slot, at : at + HALF, :] = high
            terms_ref[slot, depth + at : depth + at + HALF, :] = low

    def multiply(band, tile):
        slot = band % 2
        table = tables_ref[band]
        both = jnp.concatenate([table, table], axis=1)
        columns = slice(tile * TILE, (tile + 1) * TILE)
        sums_ref[slot, :, columns] = jnp.dot(both, terms_ref[slot, :, columns], preferred_element_type=jnp.float32)

    def drain(band, start):
        slot = band % 2
        total = sums_ref[slot, start : start + 8, :]
        for coarse in range(1, COARSE):
            at = coarse * NDELAY + start
            total = total + later(sums_ref[slot, at : at + 8, :], coarse * FINE)
        total = total * SUB_CH ** (-0.5)
        for block in range(blocks):
            at = band * NDELAY + start
            rows_ref[block, at : at + 8, :] = total[:, block * BLOCK : (block + 1) * BLOCK]

    delays.wait()
    for band in range(bands):
        tabulate(band)
    tiles = samples // TILE
    for step in range(bands + 2):
        if step < bands:
            large[step].wait()
        for tile in range(tiles):
            if step < bands:
                for fine in range(tile * FINE // tiles, (tile + 1) * FINE // tiles):
                    if fine < FINE - PAIRED:
                        fill(step, fine)
                    elif (fine - FINE + PAIRED) % 2 == 0:
                        move_pair(step, (fine - FINE + PAIRED) // 2)
            if 1 <= step <= bands:
                multiply(step - 1, tile)
            if step >= 2:
                for start in range(0, NDELAY, 8):
                    if (start // 8 + 1) * tiles // (NDELAY // 8) - 1 == tile:
                        drain(step - 2, start)

    bases.wait()
    place = lax.broadcasted_iota(jnp.int32, (2 * SPAN, BLOCK), 0)
    for side, target in ((1, give_ref), (0, keep_ref)):
        for distance in range(chips):
            owner = partner(chip, distance) * CORES + (core + side) % CORES
            begins = [band * NDELAY + base_ref[band, owner] for band in range(bands)]
            for block in range(blocks):
                pairs = []
                for band in range(0, bands, 2):
                    upper = rows_ref[block, pl.ds(begins[band], 2 * SPAN), :]
                    lower = rows_ref[block, pl.ds(begins[band + 1] - SPAN, 2 * SPAN), :]
                    pairs.append(jnp.where(place < SPAN, upper, lower))
                picked = jnp.concatenate(pairs, axis=0).astype(jnp.bfloat16)
                target[distance * count : (distance + 1) * count, block * BLOCK : (block + 1) * BLOCK] = picked


def tables_kernel(offset_ref, shift_in, length_in, picker_ref, shift_ref, length_ref, ones_ref, *, bands):
    me = lax.axis_index("chan")
    chip, core = me // CORES, me % CORES
    subbands = offset_ref.shape[1]
    place = lax.broadcasted_iota(jnp.int32, (subbands, subbands * SPAN), 1) // SPAN
    side = place // bands % CORES
    spread = (partner(chip, place // (bands * CORES)) * CORES + (core + side) % CORES) * bands + place % bands
    spread = (spread == lax.broadcasted_iota(jnp.int32, (subbands, subbands * SPAN), 0)).astype(jnp.bfloat16)
    wide = jnp.dot(offset_ref[...].astype(jnp.bfloat16), spread, preferred_element_type=jnp.float32)
    span_of = (lax.broadcasted_iota(jnp.int32, wide.shape, 1) % SPAN).astype(jnp.float32)
    picker_ref[...] = jnp.where(wide == span_of, 1.0, 0.0).astype(jnp.bfloat16)
    shift_ref[...] = jnp.broadcast_to(column(shift_in[...], shift_ref.shape[0]), shift_ref.shape)
    length_ref[...] = jnp.broadcast_to(column(length_in[...], length_ref.shape[0]), length_ref.shape)
    row = lax.broadcasted_iota(jnp.int32, ones_ref.shape, 0) % BLOCK
    lane = lax.broadcasted_iota(jnp.int32, ones_ref.shape, 1)
    ones_ref[...] = jnp.where((row < lane) | (lane >= BLOCK), 1.0, 0.0).astype(jnp.bfloat16)


def join_kernel(keep_ref, got_ref, *parts):
    count = parts[0].shape[0] // CORES
    for distance, part in zip(order(len(parts) + 1), parts):
        rows = slice(distance * count, (distance + 1) * count)
        part[:count, :] = keep_ref[rows, :]
        part[count:, :] = got_ref[rows, :]


def scores_kernel(keep_ref, got_ref, picker_ref, shift_ref, length_ref, ones_ref, *rest):
    *parts, out_hbm, prefix_ref, after_ref, out_ref, sems = rest
    trials, templates, samples = out_ref.shape
    blocks = samples // BLOCK
    subbands = picker_ref.shape[1] // SPAN
    count = parts[0].shape[0] // CORES
    near = dict(zip(order(len(parts) + 1), parts))
    stacked = [keep_ref[:count, :], got_ref[:count, :]] + [near[distance][...] for distance in sorted(near)]
    stacked = jnp.concatenate(stacked, axis=0)
    summed = jnp.dot(picker_ref[...], stacked, preferred_element_type=jnp.float32) * subbands ** (-0.5)
    current = [summed[:, b * BLOCK : (b + 1) * BLOCK] for b in range(blocks)]
    shift = shift_ref[...]
    bit = 1
    while bit < blocks:
        taken = (shift & bit) != 0
        current = [jnp.where(taken, current[b + bit] if b + bit < blocks else 0.0, current[b]) for b in range(blocks)]
        bit *= 2
    whole = jnp.concatenate(current, axis=0)
    high = whole.astype(jnp.bfloat16)
    rest = whole - high.astype(jnp.float32)
    middle = rest.astype(jnp.bfloat16)
    low = (rest - middle.astype(jnp.float32)).astype(jnp.bfloat16)
    both = jnp.dot(jnp.concatenate([high, middle, low], axis=1), ones_ref[...], preferred_element_type=jnp.float32)
    for b in range(blocks):
        columns = slice(b * BLOCK, (b + 1) * BLOCK)
        prefix_ref[:, columns] = both[b * trials : (b + 1) * trials, :BLOCK]
        after = both[b * trials : (b + 1) * trials, BLOCK:]
        if b + 1 < blocks:
            after = after + both[(b + 1) * trials : (b + 2) * trials, :BLOCK]
        after_ref[:, columns] = after
    length = length_ref[...]
    lane = lax.broadcasted_iota(jnp.int32, (templates, BLOCK), 1)
    source = (lane + length) % BLOCK
    from_next = lane < length
    weight = lax.rsqrt(length.astype(jnp.float32))
    chunk = trials // sems.shape[0]
    copies = []
    for j in range(trials):
        for b in range(blocks):
            columns = slice(b * BLOCK, (b + 1) * BLOCK)
            here = jnp.broadcast_to(prefix_ref[j : j + 1, columns], (templates, BLOCK))
            there = jnp.broadcast_to(after_ref[j : j + 1, columns], (templates, BLOCK))
            ends = jnp.take_along_axis(jnp.where(from_next, there, here), source, axis=1)
            out_ref[j, :, columns] = (ends - here) * weight
        if (j + 1) % chunk == 0:
            part = pl.ds(j + 1 - chunk, chunk)
            copies.append(pltpu.make_async_copy(out_ref.at[part], out_hbm.at[part], sems.at[len(copies)]))
            copies[-1].start()
    for copy in copies:
        copy.wait()


def order(chips):
    if chips == len(ORDER) + 1:
        return ORDER
    return tuple(range(1, chips))


def local(spectra, chan_delay, window_base, trial_offset, shift_blocks, template_len):
    channels, samples = spectra.shape
    owners = window_base.shape[0]
    bands = channels // SUB_CH
    trials, subbands = trial_offset.shape
    templates = template_len.shape[0]
    count = bands * SPAN
    chips = owners // CORES
    depth = FINE * SUB_CH
    anywhere = pl.BlockSpec(memory_space=pltpu.HBM)
    inside = pl.BlockSpec(memory_space=pltpu.VMEM)
    limits = pltpu.CompilerParams(vmem_limit_bytes=24 * 1024 * 1024)
    arrays = [
        pltpu.with_memory_space_constraint(array, pltpu.HBM)
        for array in (spectra, chan_delay.T, window_base.T, trial_offset, shift_blocks.reshape(1, trials), template_len.reshape(1, templates))
    ]
    keep, give = pl.pallas_call(
        rows_kernel,
        out_shape=[pltpu.VMEM((chips * count, samples), jnp.bfloat16)] * 2,
        in_specs=[anywhere] * 3,
        scratch_shapes=[
            pltpu.VMEM((channels, samples), jnp.float32),
            pltpu.VMEM((NDELAY, channels), jnp.int32),
            pltpu.SMEM((bands, owners), jnp.int32),
            pltpu.VMEM((2 * BLOCK, PAIRED * BLOCK), jnp.bfloat16),
            pltpu.VMEM((bands, COARSE * NDELAY, depth), jnp.bfloat16),
            pltpu.VMEM((2, 2 * depth, samples), jnp.bfloat16),
            pltpu.VMEM((2, COARSE * NDELAY, samples), jnp.float32),
            pltpu.VMEM((samples // BLOCK, bands * NDELAY + 2 * SPAN, BLOCK), jnp.float32),
            pltpu.SemaphoreType.DMA((bands + 2,)),
        ],
        compiler_params=limits,
        name="rows",
    )(*arrays[:3])
    picker, shift, length, ones = pl.pallas_call(
        functools.partial(tables_kernel, bands=bands),
        out_shape=(
            pltpu.VMEM((trials, subbands * SPAN), jnp.bfloat16),
            pltpu.VMEM((trials, BLOCK), jnp.int32),
            pltpu.VMEM((templates, BLOCK), jnp.int32),
            pltpu.VMEM((3 * BLOCK, 2 * BLOCK), jnp.bfloat16),
        ),
        compiler_params=limits,
        name="tables",
    )(*arrays[3:])
    devices = range(owners)
    got = lax.ppermute(give, "chan", [(i, i ^ 1) for i in devices])
    got = pltpu.with_memory_space_constraint(got, pltpu.VMEM)
    parts = pl.pallas_call(
        join_kernel,
        out_shape=[pltpu.VMEM((CORES * count, samples), jnp.bfloat16)] * (chips - 1),
        in_specs=[inside] * 2,
        compiler_params=limits,
        name="join",
    )(keep, got)
    arrived = []
    for distance, part in zip(order(chips), parts):
        part = lax.ppermute(part, "chan", [(i, partner(i // CORES, distance) * CORES + i % CORES) for i in devices])
        arrived.append(pltpu.with_memory_space_constraint(part, pltpu.VMEM))
    return pl.pallas_call(
        scores_kernel,
        out_shape=jax.ShapeDtypeStruct((trials, templates, samples), jnp.float32),
        in_specs=[inside] * (6 + len(arrived)),
        out_specs=anywhere,
        scratch_shapes=[
            pltpu.VMEM((trials, samples), jnp.float32),
            pltpu.VMEM((trials, samples), jnp.float32),
            pltpu.VMEM((trials, templates, samples), jnp.float32),
            pltpu.SemaphoreType.DMA((4,)),
        ],
        compiler_params=limits,
        name="scores",
    )(keep, got, picker, shift, length, ones, *arrived)


def solution(mesh):
    in_specs = (
        P(("beam", "chan"), None),
        P("chan", None),
        P(None, "chan"),
        P("chan", None),
        P("chan"),
        P(),
    )
    out_specs = P(("beam", "chan"), None, None)

    return jax.shard_map(local, mesh=mesh, in_specs=in_specs, out_specs=out_specs, check_vma=False)
```

```python
import functools

import jax
import jax.numpy as jnp
from jax import lax
from jax.experimental import pallas as pl
from jax.experimental.pallas import tpu as pltpu
from jax.sharding import PartitionSpec as P


SUB_CH = 32
NDELAY = 32
MAXD = 64
SPAN = 4
BLOCK = 128
FINE = 8
COARSE = MAXD // FINE
PAIRED = 2
TILE = 256
HALF = 16
CORES = 2
ORDER = (4, 5, 3, 7, 6, 2, 1)


def later(x, amount):
    if amount == 0:
        return x
    moved = pltpu.roll(x, amount, 1)
    lane = lax.broadcasted_iota(jnp.int32, (x.shape[0], BLOCK), 1)
    first = jnp.where(lane >= amount, moved[:, :BLOCK], jnp.zeros((), x.dtype))
    return jnp.concatenate([first, moved[:, BLOCK:]], axis=1)


def partner(chip, distance):
    return chip ^ distance


def column(row, size):
    same = lax.broadcasted_iota(jnp.int32, (size, size), 0) == lax.broadcasted_iota(jnp.int32, (size, size), 1)
    return jnp.sum(jnp.where(same, row.astype(jnp.float32), 0.0), axis=1, keepdims=True).astype(jnp.int32)


def rows_kernel(
    spectra_hbm, delay_hbm, base_hbm, rows_ref, give_ref,
    spectra_ref, delay_ref, base_ref, moves_ref, tables_ref, terms_ref, sums_ref, sems,
):
    channels, samples = spectra_ref.shape
    bands = channels // SUB_CH
    depth = FINE * SUB_CH
    blocks = samples // BLOCK

    large = []
    for band in range(bands):
        part = pl.ds(band * SUB_CH, SUB_CH)
        large.append(pltpu.make_async_copy(spectra_hbm.at[part], spectra_ref.at[part], sems.at[band]))
    delays = pltpu.make_async_copy(delay_hbm, delay_ref, sems.at[bands])
    bases = pltpu.make_async_copy(base_hbm, base_ref, sems.at[bands + 1])
    delays.start()
    large[0].start()
    for copy in large[1:]:
        copy.start()
    bases.start()
    rows_ref[:, bands * NDELAY :, :] = jnp.zeros((blocks, rows_ref.shape[1] - bands * NDELAY, BLOCK), jnp.float32)

    row = lax.broadcasted_iota(jnp.int32, (2 * BLOCK, 2 * BLOCK), 0)
    lane = lax.broadcasted_iota(jnp.int32, (2 * BLOCK, 2 * BLOCK), 1)
    for pair in range(PAIRED // 2):
        fine = FINE - PAIRED + 2 * pair + lane // BLOCK
        move = jnp.where(row == BLOCK + lane % BLOCK - fine, 1.0, 0.0)
        moves_ref[:, pair * 2 * BLOCK : (pair + 1) * 2 * BLOCK] = move.astype(jnp.bfloat16)

    def move_pair(band, pair):
        slot = band % 2
        pieces = []
        for block in range(blocks):
            for start in (0, depth):
                now = terms_ref[slot, start : start + SUB_CH, block * BLOCK : (block + 1) * BLOCK]
                if block:
                    earlier = terms_ref[slot, start : start + SUB_CH, (block - 1) * BLOCK : block * BLOCK]
                else:
                    earlier = jnp.zeros_like(now)
                pieces.append(jnp.concatenate([earlier, now], axis=1))
        moved = jnp.dot(
            jnp.concatenate(pieces, axis=0), moves_ref[:, pair * 2 * BLOCK : (pair + 1) * 2 * BLOCK], preferred_element_type=jnp.float32
        ).astype(jnp.bfloat16)
        for block in range(blocks):
            for term, start in enumerate((0, depth)):
                rows = slice((2 * block + term) * SUB_CH, (2 * block + term + 1) * SUB_CH)
                for side in range(2):
                    at = start + (FINE - PAIRED + 2 * pair + side) * SUB_CH
                    piece = moved[rows, side * BLOCK : (side + 1) * BLOCK]
                    terms_ref[slot, at : at + SUB_CH, block * BLOCK : (block + 1) * BLOCK] = piece

    def tabulate(band):
        lane = lax.broadcasted_iota(jnp.int32, (NDELAY, channels), 1)
        tiled = jnp.where(lane // SUB_CH == band, delay_ref[...], 0)
        step = SUB_CH
        while step < channels:
            tiled = tiled + pltpu.roll(tiled, step, 1)
            step *= 2
        for coarse in range(COARSE):
            for start in range(0, FINE, bands):
                wanted = coarse * FINE + start + lane // SUB_CH
                table = jnp.where(tiled == wanted, 1.0, 0.0).astype(jnp.bfloat16)
                tables_ref[band, coarse * NDELAY : (coarse + 1) * NDELAY, start * SUB_CH : start * SUB_CH + channels] = table

    def fill(band, fine):
        slot = band % 2
        for start in range(0, SUB_CH, HALF):
            at = fine * SUB_CH + start
            if fine == 0:
                first = spectra_ref[band * SUB_CH + start : band * SUB_CH + start + HALF, :]
                high = first.astype(jnp.bfloat16)
                low = (first - high.astype(jnp.float32)).astype(jnp.bfloat16)
            else:
                high = later(terms_ref[slot, start : start + HALF, :], fine)
                low = later(terms_ref[slot, depth + start : depth + start + HALF, :], fine)
            terms_ref[slot, at : at + HALF, :] = high
            terms_ref[slot, depth + at : depth + at + HALF, :] = low

    def multiply(band, tile):
        slot = band % 2
        table = tables_ref[band]
        both = jnp.concatenate([table, table], axis=1)
        columns = slice(tile * TILE, (tile + 1) * TILE)
        sums_ref[slot, :, columns] = jnp.dot(both, terms_ref[slot, :, columns], preferred_element_type=jnp.float32)

    def drain(band, start):
        slot = band % 2
        total = sums_ref[slot, start : start + 8, :]
        for coarse in range(1, COARSE):
            at = coarse * NDELAY + start
            total = total + later(sums_ref[slot, at : at + 8, :], coarse * FINE)
        total = total * SUB_CH ** (-0.5)
        for block in range(blocks):
            at = band * NDELAY + start
            rows_ref[block, at : at + 8, :] = total[:, block * BLOCK : (block + 1) * BLOCK]

    delays.wait()
    for band in range(bands):
        tabulate(band)
    tiles = samples // TILE
    for step in range(bands + 2):
        if step < bands:
            large[step].wait()
        for tile in range(tiles):
            if step < bands:
                for fine in range(tile * FINE // tiles, (tile + 1) * FINE // tiles):
                    if fine < FINE - PAIRED:
                        fill(step, fine)
                    elif (fine - FINE + PAIRED) % 2 == 0:
                        move_pair(step, (fine - FINE + PAIRED) // 2)
            if 1 <= step <= bands:
                multiply(step - 1, tile)
            if step >= 2:
                for start in range(0, NDELAY, 8):
                    if (start // 8 + 1) * tiles // (NDELAY // 8) - 1 == tile:
                        drain(step - 2, start)

    bases.wait()
    pick_windows(rows_ref, base_ref, give_ref, 1)


def pick_windows(rows_ref, base_ref, target, side):
    me = lax.axis_index("chan")
    chip, core = me // CORES, me % CORES
    bands, owners = base_ref.shape
    count = bands * SPAN
    place = lax.broadcasted_iota(jnp.int32, (2 * SPAN, BLOCK), 0)
    for distance in range(owners // CORES):
        owner = partner(chip, distance) * CORES + (core + side) % CORES
        begins = [band * NDELAY + base_ref[band, owner] for band in range(bands)]
        for block in range(rows_ref.shape[0]):
            pairs = []
            for band in range(0, bands, 2):
                upper = rows_ref[block, pl.ds(begins[band], 2 * SPAN), :]
                lower = rows_ref[block, pl.ds(begins[band + 1] - SPAN, 2 * SPAN), :]
                pairs.append(jnp.where(place < SPAN, upper, lower))
            picked = jnp.concatenate(pairs, axis=0).astype(jnp.bfloat16)
            target[distance * count : (distance + 1) * count, block * BLOCK : (block + 1) * BLOCK] = picked


def keep_kernel(rows_ref, base_hbm, keep_ref, base_ref, sem):
    copy = pltpu.make_async_copy(base_hbm, base_ref, sem)
    copy.start()
    copy.wait()
    pick_windows(rows_ref, base_ref, keep_ref, 0)


def tables_kernel(offset_ref, shift_in, length_in, picker_ref, shift_ref, length_ref, ones_ref, *, bands):
    me = lax.axis_index("chan")
    chip, core = me // CORES, me % CORES
    subbands = offset_ref.shape[1]
    place = lax.broadcasted_iota(jnp.int32, (subbands, subbands * SPAN), 1) // SPAN
    side = place // bands % CORES
    spread = (partner(chip, place // (bands * CORES)) * CORES + (core + side) % CORES) * bands + place % bands
    spread = (spread == lax.broadcasted_iota(jnp.int32, (subbands, subbands * SPAN), 0)).astype(jnp.bfloat16)
    wide = jnp.dot(offset_ref[...].astype(jnp.bfloat16), spread, preferred_element_type=jnp.float32)
    span_of = (lax.broadcasted_iota(jnp.int32, wide.shape, 1) % SPAN).astype(jnp.float32)
    picker_ref[...] = jnp.where(wide == span_of, 1.0, 0.0).astype(jnp.bfloat16)
    shift_ref[...] = jnp.broadcast_to(column(shift_in[...], shift_ref.shape[0]), shift_ref.shape)
    length_ref[...] = jnp.broadcast_to(column(length_in[...], length_ref.shape[0]), length_ref.shape)
    row = lax.broadcasted_iota(jnp.int32, ones_ref.shape, 0) % BLOCK
    lane = lax.broadcasted_iota(jnp.int32, ones_ref.shape, 1)
    ones_ref[...] = jnp.where((row < lane) | (lane >= BLOCK), 1.0, 0.0).astype(jnp.bfloat16)


def join_kernel(keep_ref, got_ref, *parts):
    count = parts[0].shape[0] // CORES
    for distance, part in zip(order(len(parts) + 1), parts):
        rows = slice(distance * count, (distance + 1) * count)
        part[:count, :] = keep_ref[rows, :]
        part[count:, :] = got_ref[rows, :]


def scores_kernel(keep_ref, got_ref, picker_ref, shift_ref, length_ref, ones_ref, *rest):
    *parts, out_hbm, prefix_ref, after_ref, out_ref, sems = rest
    trials, templates, samples = out_ref.shape
    blocks = samples // BLOCK
    subbands = picker_ref.shape[1] // SPAN
    count = parts[0].shape[0] // CORES
    near = dict(zip(order(len(parts) + 1), parts))
    stacked = [keep_ref[:count, :], got_ref[:count, :]] + [near[distance][...] for distance in sorted(near)]
    stacked = jnp.concatenate(stacked, axis=0)
    summed = jnp.dot(picker_ref[...], stacked, preferred_element_type=jnp.float32) * subbands ** (-0.5)
    current = [summed[:, b * BLOCK : (b + 1) * BLOCK] for b in range(blocks)]
    shift = shift_ref[...]
    bit = 1
    while bit < blocks:
        taken = (shift & bit) != 0
        current = [jnp.where(taken, current[b + bit] if b + bit < blocks else 0.0, current[b]) for b in range(blocks)]
        bit *= 2
    whole = jnp.concatenate(current, axis=0)
    high = whole.astype(jnp.bfloat16)
    rest = whole - high.astype(jnp.float32)
    middle = rest.astype(jnp.bfloat16)
    low = (rest - middle.astype(jnp.float32)).astype(jnp.bfloat16)
    both = jnp.dot(jnp.concatenate([high, middle, low], axis=1), ones_ref[...], preferred_element_type=jnp.float32)
    for b in range(blocks):
        columns = slice(b * BLOCK, (b + 1) * BLOCK)
        prefix_ref[:, columns] = both[b * trials : (b + 1) * trials, :BLOCK]
        after = both[b * trials : (b + 1) * trials, BLOCK:]
        if b + 1 < blocks:
            after = after + both[(b + 1) * trials : (b + 2) * trials, :BLOCK]
        after_ref[:, columns] = after
    length = length_ref[...]
    lane = lax.broadcasted_iota(jnp.int32, (templates, BLOCK), 1)
    source = (lane + length) % BLOCK
    from_next = lane < length
    weight = lax.rsqrt(length.astype(jnp.float32))
    chunk = trials // sems.shape[0]
    copies = []
    for j in range(trials):
        for b in range(blocks):
            columns = slice(b * BLOCK, (b + 1) * BLOCK)
            here = jnp.broadcast_to(prefix_ref[j : j + 1, columns], (templates, BLOCK))
            there = jnp.broadcast_to(after_ref[j : j + 1, columns], (templates, BLOCK))
            ends = jnp.take_along_axis(jnp.where(from_next, there, here), source, axis=1)
            out_ref[j, :, columns] = (ends - here) * weight
        if (j + 1) % chunk == 0:
            part = pl.ds(j + 1 - chunk, chunk)
            copies.append(pltpu.make_async_copy(out_ref.at[part], out_hbm.at[part], sems.at[len(copies)]))
            copies[-1].start()
    for copy in copies:
        copy.wait()


def order(chips):
    if chips == len(ORDER) + 1:
        return ORDER
    return tuple(range(1, chips))


def local(spectra, chan_delay, window_base, trial_offset, shift_blocks, template_len):
    channels, samples = spectra.shape
    owners = window_base.shape[0]
    bands = channels // SUB_CH
    trials, subbands = trial_offset.shape
    templates = template_len.shape[0]
    count = bands * SPAN
    chips = owners // CORES
    depth = FINE * SUB_CH
    anywhere = pl.BlockSpec(memory_space=pltpu.HBM)
    inside = pl.BlockSpec(memory_space=pltpu.VMEM)
    limits = pltpu.CompilerParams(vmem_limit_bytes=24 * 1024 * 1024)
    arrays = [
        pltpu.with_memory_space_constraint(array, pltpu.HBM)
        for array in (spectra, chan_delay.T, window_base.T, trial_offset, shift_blocks.reshape(1, trials), template_len.reshape(1, templates))
    ]
    rows, give = pl.pallas_call(
        rows_kernel,
        out_shape=(
            pltpu.VMEM((samples // BLOCK, bands * NDELAY + 2 * SPAN, BLOCK), jnp.float32),
            pltpu.VMEM((chips * count, samples), jnp.bfloat16),
        ),
        in_specs=[anywhere] * 3,
        scratch_shapes=[
            pltpu.VMEM((channels, samples), jnp.float32),
            pltpu.VMEM((NDELAY, channels), jnp.int32),
            pltpu.SMEM((bands, owners), jnp.int32),
            pltpu.VMEM((2 * BLOCK, PAIRED * BLOCK), jnp.bfloat16),
            pltpu.VMEM((bands, COARSE * NDELAY, depth), jnp.bfloat16),
            pltpu.VMEM((2, 2 * depth, samples), jnp.bfloat16),
            pltpu.VMEM((2, COARSE * NDELAY, samples), jnp.float32),
            pltpu.SemaphoreType.DMA((bands + 2,)),
        ],
        compiler_params=limits,
        name="rows",
    )(*arrays[:3])
    picker, shift, length, ones = pl.pallas_call(
        functools.partial(tables_kernel, bands=bands),
        out_shape=(
            pltpu.VMEM((trials, subbands * SPAN), jnp.bfloat16),
            pltpu.VMEM((trials, BLOCK), jnp.int32),
            pltpu.VMEM((templates, BLOCK), jnp.int32),
            pltpu.VMEM((3 * BLOCK, 2 * BLOCK), jnp.bfloat16),
        ),
        compiler_params=limits,
        name="tables",
    )(*arrays[3:])
    devices = range(owners)
    got = lax.ppermute(give, "chan", [(i, i ^ 1) for i in devices])
    keep = pl.pallas_call(
        keep_kernel,
        out_shape=pltpu.VMEM((chips * count, samples), jnp.bfloat16),
        in_specs=[inside, anywhere],
        scratch_shapes=[pltpu.SMEM((bands, owners), jnp.int32), pltpu.SemaphoreType.DMA],
        compiler_params=limits,
        name="keep",
    )(rows, arrays[2])
    got = pltpu.with_memory_space_constraint(got, pltpu.VMEM)
    parts = pl.pallas_call(
        join_kernel,
        out_shape=[pltpu.VMEM((CORES * count, samples), jnp.bfloat16)] * (chips - 1),
        in_specs=[inside] * 2,
        compiler_params=limits,
        name="join",
    )(keep, got)
    arrived = []
    for distance, part in zip(order(chips), parts):
        part = lax.ppermute(part, "chan", [(i, partner(i // CORES, distance) * CORES + i % CORES) for i in devices])
        arrived.append(pltpu.with_memory_space_constraint(part, pltpu.VMEM))
    return pl.pallas_call(
        scores_kernel,
        out_shape=jax.ShapeDtypeStruct((trials, templates, samples), jnp.float32),
        in_specs=[inside] * (6 + len(arrived)),
        out_specs=anywhere,
        scratch_shapes=[
            pltpu.VMEM((trials, samples), jnp.float32),
            pltpu.VMEM((trials, samples), jnp.float32),
            pltpu.VMEM((trials, templates, samples), jnp.float32),
            pltpu.SemaphoreType.DMA((4,)),
        ],
        compiler_params=limits,
        name="scores",
    )(keep, got, picker, shift, length, ones, *arrived)


def solution(mesh):
    in_specs = (
        P(("beam", "chan"), None),
        P("chan", None),
        P(None, "chan"),
        P("chan", None),
        P("chan"),
        P(),
    )
    out_specs = P(("beam", "chan"), None, None)

    return jax.shard_map(local, mesh=mesh, in_specs=in_specs, out_specs=out_specs, check_vma=False)
```
